8 devices in a mesh: dp: 1 (over z), tp: 2 (over y), ep: 4 (over x, core).
Axes of the slice: x: 2, y: 2, z: 1, core: 2. Of those that a mesh axis runs over, the one named last changes fastest.
Arguments:
- hidden: bfloat16 [2048, 1024], P(('dp', 'ep'))
- k_cache: bfloat16 [2048, 256, 8, 64], P(('dp', 'ep'), None, 'tp')
- v_cache: bfloat16 [2048, 256, 8, 64], P(('dp', 'ep'), None, 'tp')
- lengths: int32 [2048], P(('dp', 'ep'))
- expert_ids: int32 [2048, 8], P(('dp', 'ep'))
- route_gates: float32 [2048, 8], P(('dp', 'ep'))
- norm_gain: float32 [1024], replicated
- w_query: bfloat16 [1024, 1024], P(None, 'tp')
- w_key: bfloat16 [1024, 512], P(None, 'tp')
- w_value: bfloat16 [1024, 512], P(None, 'tp')
- w_out: bfloat16 [1024, 1024], P('tp')
- ws_gate: bfloat16 [1024, 512], P(None, 'tp')
- ws_up: bfloat16 [1024, 512], P(None, 'tp')
- ws_down: bfloat16 [512, 1024], P('tp')
- we_gate: bfloat16 [32, 1024, 512], P(('ep', 'tp'))
- we_up: bfloat16 [32, 1024, 512], P(('ep', 'tp'))
- we_down: bfloat16 [32, 512, 1024], P(('ep', 'tp'))
Outputs:
- output: bfloat16 [2048, 1024], P(('dp', 'ep'))
All inputs are finite; a program needn't handle non-finite values.
Results may differ from the reference program's by a relative error of at most 0.0063324.
Values are sent between devices in bfloat16 or wider.
A program may use at most 1 GiB of HBM per device.

```python
import jax
import jax.numpy as jnp
from jax import lax

TOKENS = 2048
EP_GROUPS = 4
D_MODEL = 1024
Q_HEADS = 16
KV_HEADS = 8
HEAD_DIM = 64
SHARED_FF = 512
NUM_EXPERTS = 32
TOP_K = 8
EXPERT_FF = 512
SEQ_LEN = 256

NORM_EPS = 1e-6
HALF_TOK = TOKENS // (2 * EP_GROUPS)
GROUP_EXPERTS = NUM_EXPERTS // EP_GROUPS
GROUP_SIZE = Q_HEADS // KV_HEADS


def draw_weight(rand_key, arr_shape, fan_in, w_gain=1.0):
    w_scale = w_gain / fan_in ** 0.5
    return (jax.random.normal(rand_key, arr_shape, jnp.float32) * w_scale).astype(jnp.bfloat16)


def draw_routing(route_key):
    sub_keys = jax.random.split(route_key, 4)
    slot_idx = jnp.arange(TOP_K)
    tok_scores = jax.random.randint(sub_keys[0], (EP_GROUPS, 2, HALF_TOK), 0, 1 << 20) * HALF_TOK + jnp.arange(HALF_TOK)
    base_chip = jnp.argsort(tok_scores, axis=-1) % EP_GROUPS
    chip_scores = jax.random.randint(sub_keys[1], (EP_GROUPS, 2, EP_GROUPS), 0, 1 << 20) * EP_GROUPS + jnp.arange(EP_GROUPS)
    chip_perm = jnp.argsort(chip_scores, axis=-1)
    offsets = chip_perm[:, :, slot_idx % EP_GROUPS]
    chip_ids = (base_chip[:, :, :, None] + offsets[:, :, None, :]) % EP_GROUPS
    local_base = jax.random.randint(sub_keys[2], (EP_GROUPS, 2, HALF_TOK, EP_GROUPS), 0, GROUP_EXPERTS)
    local_idx = (local_base[:, :, :, slot_idx % EP_GROUPS] + slot_idx // EP_GROUPS) % GROUP_EXPERTS
    expert_ids = (chip_ids * GROUP_EXPERTS + local_idx).reshape(TOKENS, TOP_K).astype(jnp.int32)
    lengths = jax.random.randint(sub_keys[3], (TOKENS,), SEQ_LEN // 4, SEQ_LEN + 1)
    lengths = lengths.at[0].set(SEQ_LEN).at[1].set(SEQ_LEN // 4).astype(jnp.int32)
    return expert_ids, lengths


def setup_inputs(seed: int = 0, part: int = 0) -> dict:
    part_key = jax.random.fold_in(jax.random.key(seed), part)
    part_keys = jax.random.split(part_key, 5)
    w_keys = jax.random.split(jax.random.key(seed + 1), 11)
    cache_shape = (TOKENS, SEQ_LEN, KV_HEADS, HEAD_DIM)
    hidden = jax.random.normal(part_keys[0], (TOKENS, D_MODEL), jnp.float32).astype(jnp.bfloat16)
    k_cache = jax.random.normal(part_keys[1], cache_shape, jnp.float32).astype(jnp.bfloat16)
    v_cache = jax.random.normal(part_keys[2], cache_shape, jnp.float32).astype(jnp.bfloat16)
    expert_ids, lengths = draw_routing(part_keys[3])
    route_gates = jax.random.uniform(part_keys[4], (TOKENS, TOP_K), jnp.float32, 0.2, 1.0) * (1.5 / TOP_K ** 0.5)
    norm_gain = jax.random.uniform(w_keys[0], (D_MODEL,), jnp.float32, 0.5, 1.5)
    q_width = Q_HEADS * HEAD_DIM
    kv_width = KV_HEADS * HEAD_DIM
    return {
        'hidden': hidden,
        'k_cache': k_cache,
        'v_cache': v_cache,
        'lengths': lengths,
        'expert_ids': expert_ids,
        'route_gates': route_gates,
        'norm_gain': norm_gain,
        'w_query': draw_weight(w_keys[1], (D_MODEL, q_width), D_MODEL),
        'w_key': draw_weight(w_keys[2], (D_MODEL, kv_width), D_MODEL),
        'w_value': draw_weight(w_keys[3], (D_MODEL, kv_width), D_MODEL),
        'w_out': draw_weight(w_keys[4], (q_width, D_MODEL), q_width, (SEQ_LEN / 16) ** 0.5),
        'ws_gate': draw_weight(w_keys[5], (D_MODEL, SHARED_FF), D_MODEL),
        'ws_up': draw_weight(w_keys[6], (D_MODEL, SHARED_FF), D_MODEL),
        'ws_down': draw_weight(w_keys[7], (SHARED_FF, D_MODEL), SHARED_FF),
        'we_gate': draw_weight(w_keys[8], (NUM_EXPERTS, D_MODEL, EXPERT_FF), D_MODEL),
        'we_up': draw_weight(w_keys[9], (NUM_EXPERTS, D_MODEL, EXPERT_FF), D_MODEL),
        'we_down': draw_weight(w_keys[10], (NUM_EXPERTS, EXPERT_FF, D_MODEL), EXPERT_FF),
    }


def rms_norm(hidden, norm_gain):
    hid_f32 = hidden.astype(jnp.float32)
    inv_rms = lax.rsqrt(jnp.mean(hid_f32 * hid_f32, axis=-1, keepdims=True) + NORM_EPS)
    return (hid_f32 * inv_rms * norm_gain).astype(jnp.bfloat16)


def attend_block(blk_args):
    q_blk, kn_blk, vn_blk, kc_blk, vc_blk, len_blk = blk_args
    score_scale = HEAD_DIM ** -0.5
    s_cache = jnp.einsum('bkgd,bskd->bkgs', q_blk, kc_blk.astype(jnp.float32)) * score_scale
    valid_pos = jnp.arange(SEQ_LEN)[None, :] < len_blk[:, None]
    s_cache = jnp.where(valid_pos[:, None, None, :], s_cache, -1e30)
    s_new = jnp.einsum('bkgd,bkd->bkg', q_blk, kn_blk) * score_scale
    peak_score = jnp.maximum(jnp.max(s_cache, axis=-1), s_new)
    p_cache = jnp.exp(s_cache - peak_score[..., None])
    p_new = jnp.exp(s_new - peak_score)
    denom_sum = jnp.sum(p_cache, axis=-1) + p_new
    p_round = p_cache.astype(jnp.bfloat16).astype(jnp.float32)
    numer_sum = jnp.einsum('bkgs,bskd->bkgd', p_round, vc_blk.astype(jnp.float32)) + p_new[..., None] * vn_blk[:, :, None, :]
    return numer_sum / denom_sum[..., None]


def reference(hidden, k_cache, v_cache, lengths, expert_ids, route_gates, norm_gain, w_query, w_key, w_value, w_out, ws_gate, ws_up, ws_down, we_gate, we_up, we_down):
    x_norm = rms_norm(hidden, norm_gain)
    n_blocks = TOKENS // 4
    q_all = jnp.dot(x_norm, w_query, preferred_element_type=jnp.float32).astype(jnp.bfloat16).astype(jnp.float32)
    k_new = jnp.dot(x_norm, w_key, preferred_element_type=jnp.float32).astype(jnp.bfloat16).astype(jnp.float32)
    v_new = jnp.dot(x_norm, w_value, preferred_element_type=jnp.float32).astype(jnp.bfloat16).astype(jnp.float32)
    blk_args = (
        q_all.reshape(n_blocks, 4, KV_HEADS, GROUP_SIZE, HEAD_DIM),
        k_new.reshape(n_blocks, 4, KV_HEADS, HEAD_DIM),
        v_new.reshape(n_blocks, 4, KV_HEADS, HEAD_DIM),
        k_cache.reshape(n_blocks, 4, SEQ_LEN, KV_HEADS, HEAD_DIM),
        v_cache.reshape(n_blocks, 4, SEQ_LEN, KV_HEADS, HEAD_DIM),
        lengths.reshape(n_blocks, 4),
    )
    heads_out = lax.map(attend_block, blk_args)
    o_flat = heads_out.reshape(TOKENS, Q_HEADS * HEAD_DIM).astype(jnp.bfloat16)
    attn_part = jnp.dot(o_flat, w_out, preferred_element_type=jnp.float32)
    gate_s = jnp.dot(x_norm, ws_gate, preferred_element_type=jnp.float32)
    up_s = jnp.dot(x_norm, ws_up, preferred_element_type=jnp.float32)
    shared = jnp.dot((jax.nn.silu(gate_s) * up_s).astype(jnp.bfloat16), ws_down, preferred_element_type=jnp.float32)
    onehot_ids = (expert_ids[:, :, None] == jnp.arange(NUM_EXPERTS)[None, None, :]).astype(jnp.float32)
    combine = jnp.sum(route_gates[:, :, None] * onehot_ids, axis=1)
    x_f32 = x_norm.astype(jnp.float32)

    def expert_step(acc_sum, exp_args):
        gate_w, up_w, down_w, gate_col = exp_args
        gate_e = jnp.dot(x_f32, gate_w.astype(jnp.float32))
        up_e = jnp.dot(x_f32, up_w.astype(jnp.float32))
        hid_e = (jax.nn.silu(gate_e) * up_e).astype(jnp.bfloat16).astype(jnp.float32)
        return acc_sum + gate_col[:, None] * jnp.dot(hid_e, down_w.astype(jnp.float32)), None

    routed = lax.scan(expert_step, jnp.zeros((TOKENS, D_MODEL), jnp.float32), (we_gate, we_up, we_down, combine.T))[0]
    return (hidden.astype(jnp.float32) + attn_part + shared + routed).astype(jnp.bfloat16)
```

```python
import functools

import jax
import jax.numpy as jnp
from jax import lax
from jax.experimental import pallas as pl
from jax.experimental.pallas import tpu as pltpu
from jax.sharding import PartitionSpec as P

NORM_EPS = 1e-6
F32 = jnp.float32
BF16 = jnp.bfloat16
MESH = pl.DeviceIdType.MESH

BLK = 16
SLOTS = 4
CHUNK = 64
HEAD_BLOCKS = 8


def layer_kernel(
    h_ref, ids_ref, gates_ref, lens_ref, gain_ref, k_hbm, v_hbm, wq_hbm, wk_hbm, wv_hbm, wo_hbm, wsg_hbm, wsu_hbm, wsd_hbm,
    weg_hbm, weu_hbm, wed_hbm,
    out_hbm,
    wq, wk, wv, wo, wsg, wsu, wsd, weg, weu, wed, kbuf, vbuf,
    h_in, ids_in, gates_in, xs, aug, oflat, acc, part, cwb,
    psend, precv, dsend, drecv, xsend, xrecv, ysend, yrecv, obuf,
    wsem, wosem, esem, ksem, vsem, hs_send, hs_recv, p_send, p_recv, d_send, d_recv, x_send, x_recv, y_send, y_recv, osem,
):
    tp = lax.axis_index("tp")
    ep = lax.axis_index("ep")
    dp = lax.axis_index("dp")
    core = lax.rem(ep, 2)
    chip = ep // 2
    partner = (dp, tp, 2 * chip + 1 - core)
    xnbr = (dp, tp, 2 * (1 - chip) + core)
    ynbr = (dp, 1 - tp, ep)

    rows = h_ref.shape[0]
    n_blocks = rows // BLK
    n_chunks = rows // CHUNK
    kv_width = wk.shape[1]
    n_local = weg.shape[0]
    n_heads = wq.shape[1] // 64
    seq_len = kbuf.shape[3]

    small = [(wq_hbm, wq), (wk_hbm, wk), (wv_hbm, wv), (wsg_hbm, wsg), (wsu_hbm, wsu), (wsd_hbm, wsd)]
    small_copies = [pltpu.make_async_copy(s, d, wsem.at[i]) for i, (s, d) in enumerate(small)]
    for c in small_copies:
        c.start()
    barrier = pltpu.get_barrier_semaphore()
    for dev in (partner, xnbr, ynbr):
        pl.semaphore_signal(barrier, inc=1, device_id=dev, device_id_type=MESH)
    big_copies = [pltpu.make_async_copy(s, d, esem.at[i]) for i, (s, d) in enumerate(((weg_hbm, weg), (weu_hbm, weu), (wed_hbm, wed)))]
    for c in big_copies:
        c.start()
    pl.semaphore_wait(barrier, 3)

    def remote(src, dst, ssem, rsem, dev):
        return pltpu.make_async_remote_copy(src_ref=src, dst_ref=dst, send_sem=ssem, recv_sem=rsem, device_id=dev, device_id_type=MESH)

    def token_copies(srcs, slot, dev):
        dsts = (h_in.at[slot], ids_in.at[slot], gates_in.at[slot])
        return [remote(s, d, hs_send.at[slot, i], hs_recv.at[slot, i], dev) for i, (s, d) in enumerate(zip(srcs, dsts))]

    own = (h_ref, ids_ref, gates_ref)
    to_partner = token_copies(own, 0, partner)
    to_xnbr = token_copies(own, 1, xnbr)
    forward = token_copies((h_in.at[1], ids_in.at[1], gates_in.at[1]), 2, partner)
    for c in to_xnbr + to_partner:
        c.start()

    wo_copies = []
    for i in range(n_heads):
        dst_row = (i % 2) * kv_width + (i // 2) * 64
        wo_copies.append(pltpu.make_async_copy(wo_hbm.at[pl.ds(i * 64, 64), :], wo.at[pl.ds(dst_row, 64), :], wosem.at[i]))

    def kv_copies(b, slot):
        start = pl.multiple_of(b * BLK, BLK)
        return (
            pltpu.make_async_copy(k_hbm.at[pl.ds(start, BLK)], kbuf.at[slot], ksem.at[slot]),
            pltpu.make_async_copy(v_hbm.at[pl.ds(start, BLK)], vbuf.at[slot], vsem.at[slot]),
        )

    def normalize(src):
        @pl.loop(0, rows // 64)
        def _(i):
            r = pl.ds(pl.multiple_of(i * 64, 64), 64)
            hf = src[r, :].astype(F32)
            inv = lax.rsqrt(jnp.mean(hf * hf, axis=1, keepdims=True) + NORM_EPS)
            xs[r, :] = (hf * inv * gain_ref[...]).astype(BF16)

    def gate_weights(ids, gates):
        first = ep * (2 * n_local) + tp * n_local
        expert = first + lax.broadcasted_iota(jnp.int32, (8, rows), 0)
        total = jnp.zeros((8, rows), F32)
        for j in range(ids.shape[0]):
            total += jnp.where(ids[j : j + 1, :] == expert, gates[j : j + 1, :], 0.0)
        cols = total.T
        for e in range(n_local):
            cwb[e] = jnp.broadcast_to(cols[:, e : e + 1], (rows, 128))

    half = rows // 2

    def experts(dst, first):
        @pl.loop(0, n_local)
        def _(e):
            for m in range(2):
                r = pl.ds(m * half, half)
                x = xs[r, :]
                gate = jnp.dot(x, weg[e], preferred_element_type=F32)
                up = jnp.dot(x, weu[e], preferred_element_type=F32)
                hid = (gate * jax.nn.sigmoid(gate) * up).astype(BF16)
                y = jnp.dot(hid, wed[e], preferred_element_type=F32)
                w = jnp.tile(cwb[e, r, :], (1, y.shape[1] // 128))
                if first:
                    @pl.when(e == 0)
                    def _():
                        dst[r, :] = w * y

                    @pl.when(e > 0)
                    def _():
                        dst[r, :] += w * y
                else:
                    dst[r, :] += w * y

    normalize(h_ref)
    for c in small_copies:
        c.wait()
    for c in wo_copies:
        c.start()
    for b in range(SLOTS):
        for c in kv_copies(b, b):
            c.start()

    col = lax.broadcasted_iota(jnp.int32, (n_heads * 64, n_heads * 64), 1)
    row = lax.broadcasted_iota(jnp.int32, (n_heads * 64, n_heads * 64), 0)
    src_row = ((lax.rem(col, kv_width) // 64) * 2 + col // kv_width) * 64 + lax.rem(col, 64)
    perm = (row == src_row).astype(F32).astype(BF16)
    lens = jnp.broadcast_to(lens_ref[...], (8, rows)).astype(F32).T
    q_w = n_heads * 64
    for m in range(2):
        r = pl.ds(m * half, half)
        x = xs[r, :]
        q = jnp.dot(x, wq[...], preferred_element_type=F32).astype(BF16)
        aug[r, 0:q_w] = jnp.dot(q, perm, preferred_element_type=F32).astype(BF16)
        aug[r, q_w : q_w + kv_width] = jnp.dot(x, wk[...], preferred_element_type=F32).astype(BF16)
        aug[r, q_w + kv_width : q_w + 2 * kv_width] = jnp.dot(x, wv[...], preferred_element_type=F32).astype(BF16)
        aug[r, q_w + 2 * kv_width : q_w + 2 * kv_width + 128] = jnp.broadcast_to(lens[m * half : (m + 1) * half, 0:1], (half, 128)).astype(BF16)
        gate = jnp.dot(x, wsg[...], preferred_element_type=F32)
        up = jnp.dot(x, wsu[...], preferred_element_type=F32)
        hid = (gate * jax.nn.sigmoid(gate) * up).astype(BF16)
        acc[r, :] = jnp.dot(hid, wsd[...], preferred_element_type=F32)

    gate_weights(ids_ref[...], gates_ref[...])
    for c in big_copies:
        c.wait()
    experts(acc, False)

    def wait_recv(copies):
        for c in copies:
            c.wait_recv()

    wait_recv(to_partner)
    normalize(h_in.at[0])
    gate_weights(ids_in[0], gates_in[0])
    experts(part, True)
    psend[...] = part[...].astype(BF16)
    partner_part = remote(psend, precv, p_send.at[0], p_recv.at[0], partner)
    partner_part.start()

    R8 = BLK * n_heads
    n_pairs = BLK // 2

    def attend(b):
        slot = lax.rem(b, SLOTS)
        for c in kv_copies(b, slot):
            c.wait()
        t = pl.ds(pl.multiple_of(b * BLK, BLK), BLK)
        rep = (lax.broadcasted_iota(jnp.int32, (R8, BLK), 0) // n_heads == lax.broadcasted_iota(jnp.int32, (R8, BLK), 1)).astype(F32).astype(BF16)
        full = jnp.dot(rep, aug[t, :], preferred_element_type=F32)
        r_i = lax.broadcasted_iota(jnp.int32, (R8, kv_width), 0)
        c_i = lax.broadcasted_iota(jnp.int32, (R8, kv_width), 1)
        own_head = lax.rem(r_i, n_heads) // 2 == c_i // 64
        even = lax.rem(r_i, 2) == 0
        qf = jnp.where(own_head, jnp.where(even, full[:, 0:kv_width], full[:, kv_width : 2 * kv_width]), 0.0)
        kn = full[:, q_w : q_w + kv_width]
        vn = full[:, q_w + kv_width : q_w + 2 * kv_width]
        ln = full[:, q_w + 2 * kv_width : q_w + 2 * kv_width + 128]
        qb = qf.astype(BF16)
        s_new = jnp.sum(qf * kn, axis=1, keepdims=True) * 0.125
        parts = []
        for p in range(n_pairs):
            lhs = qb[16 * p : 16 * p + 16]
            parts.append(jnp.dot(lhs, kbuf[slot, 2 * p], preferred_element_type=F32)[0:8])
            parts.append(jnp.dot(lhs, kbuf[slot, 2 * p + 1], preferred_element_type=F32)[8:16])
        s = jnp.concatenate(parts, axis=0) * 0.125
        pos = lax.broadcasted_iota(jnp.int32, (R8, seq_len), 1).astype(F32)
        s = jnp.where(pos < jnp.tile(ln, (1, seq_len // 128)), s, -1e30)
        top = jnp.maximum(jnp.max(s, axis=1, keepdims=True), s_new)
        w = jnp.exp(s - top)
        w_new = jnp.exp(s_new - top)
        den = jnp.sum(w, axis=1, keepdims=True) + w_new
        wb = w.astype(BF16)
        parts = []
        nt = (((1,), (1,)), ((), ()))
        for p in range(n_pairs):
            lhs = wb[16 * p : 16 * p + 16]
            parts.append(lax.dot_general(lhs, vbuf[slot, 2 * p], nt, preferred_element_type=F32)[0:8])
            parts.append(lax.dot_general(lhs, vbuf[slot, 2 * p + 1], nt, preferred_element_type=F32)[8:16])
        num = jnp.concatenate(parts, axis=0) + w_new * vn
        o = jnp.where(own_head, num / den, 0.0).astype(BF16)
        g_r = lax.broadcasted_iota(jnp.int32, (2 * BLK, R8), 0)
        g_c = lax.broadcasted_iota(jnp.int32, (2 * BLK, R8), 1)
        fold = ((g_c // n_heads == lax.rem(g_r, BLK)) & (lax.rem(g_c, 2) == g_r // BLK)).astype(F32).astype(BF16)
        folded = jnp.dot(fold, o, preferred_element_type=F32).astype(BF16)
        oflat[t, 0:kv_width] = folded[0:BLK]
        oflat[t, kv_width : 2 * kv_width] = folded[BLK : 2 * BLK]

    def attend_and_refill(b):
        attend(b)

        @pl.when(b + SLOTS < n_blocks)
        def _():
            for c in kv_copies(b + SLOTS, lax.rem(b, SLOTS)):
                c.start()

    @pl.loop(0, HEAD_BLOCKS)
    def _(b):
        attend_and_refill(b)

    wait_recv(to_xnbr)
    for c in forward:
        c.start()
    normalize(h_in.at[1])
    gate_weights(ids_in[1], gates_in[1])
    experts(part, True)
    partner_part.wait_recv()

    wait_recv(forward)
    normalize(h_in.at[2])
    gate_weights(ids_in[2], gates_in[2])

    @pl.loop(0, n_chunks)
    def _(c):
        r = pl.ds(pl.multiple_of(c * CHUNK, CHUNK), CHUNK)
        acc[r, :] += precv[r, :].astype(F32)
        xpart = part[r, :]
        obuf[r, :] = xpart

    experts(part, True)
    dsend[...] = part[...].astype(BF16)
    diag_part = remote(dsend, drecv, d_send.at[0], d_recv.at[0], partner)
    diag_part.start()
    diag_part.wait_recv()

    def chunk_copy(src, dst, ssem, rsem, c, dev):
        r = pl.ds(pl.multiple_of(c * CHUNK, CHUNK), CHUNK)
        return remote(src.at[r, :], dst.at[r, :], ssem.at[c], rsem.at[c], dev)

    @pl.loop(0, n_chunks)
    def _(c):
        r = pl.ds(pl.multiple_of(c * CHUNK, CHUNK), CHUNK)
        xsend[r, :] = (obuf[r, :] + drecv[r, :].astype(F32)).astype(BF16)
        chunk_copy(xsend, xrecv, x_send, x_recv, c, xnbr).start()

    for c in wo_copies:
        c.wait()

    def finish(c):
        r = pl.ds(pl.multiple_of(c * CHUNK, CHUNK), CHUNK)
        chunk_copy(ysend, yrecv, y_send, y_recv, c, ynbr).wait_recv()
        both = ysend[r, :].astype(F32) + yrecv[r, :].astype(F32)
        xs[r, :] = (h_ref[r, :].astype(F32) + both).astype(BF16)
        pltpu.make_async_copy(xs.at[r, :], out_hbm.at[r, :], osem.at[c]).start()

    per_chunk = (n_blocks - HEAD_BLOCKS) // n_chunks

    @pl.loop(0, n_chunks)
    def _(c):
        @pl.loop(0, per_chunk)
        def _(i):
            attend_and_refill(HEAD_BLOCKS + c * per_chunk + i)

        r = pl.ds(pl.multiple_of(c * CHUNK, CHUNK), CHUNK)
        attn = jnp.dot(oflat[r, :], wo[...], preferred_element_type=F32)
        chunk_copy(xsend, xrecv, x_send, x_recv, c, xnbr).wait_recv()
        ysend[r, :] = (acc[r, :] + attn + xrecv[r, :].astype(F32)).astype(BF16)
        chunk_copy(ysend, yrecv, y_send, y_recv, c, ynbr).start()

        @pl.when(c > 0)
        def _():
            finish(c - 1)

    finish(n_chunks - 1)

    for c in to_partner + to_xnbr + forward + [partner_part, diag_part]:
        c.wait_send()

    @pl.loop(0, n_chunks)
    def _(c):
        r = pl.ds(pl.multiple_of(c * CHUNK, CHUNK), CHUNK)
        chunk_copy(xsend, xrecv, x_send, x_recv, c, xnbr).wait_send()
        chunk_copy(ysend, yrecv, y_send, y_recv, c, ynbr).wait_send()
        pltpu.make_async_copy(xs.at[r, :], out_hbm.at[r, :], osem.at[c]).wait()


def solution(mesh):
    tok_rows = P(("dp", "ep"), None)
    cache_spec = P(("dp", "ep"), None, "tp", None)
    col_split = P(None, "tp")
    row_split = P("tp", None)
    exp_split = P(("ep", "tp"), None, None)
    in_specs = (tok_rows, cache_spec, cache_spec, P(("dp", "ep")), tok_rows, tok_rows, P(None), col_split, col_split, col_split, row_split, col_split, col_split, row_split, exp_split, exp_split, exp_split)

    def device_body(hidden, k_cache, v_cache, lengths, expert_ids, route_gates, norm_gain, w_query, w_key, w_value, w_out, ws_gate, ws_up, ws_down, we_gate, we_up, we_down):
        rows, width = hidden.shape
        seq_len, kv_local, head_dim = k_cache.shape[1:]
        kv_width = kv_local * head_dim
        top_k = expert_ids.shape[1]
        k_t = k_cache.transpose(0, 2, 3, 1).reshape(rows, kv_width, seq_len)
        v_t = v_cache.transpose(0, 2, 3, 1).reshape(rows, kv_width, seq_len)
        n_chunks = rows // CHUNK
        q_w = w_query.shape[1]
        dma = pltpu.SemaphoreType.DMA
        vmem = pltpu.VMEM
        scratch = [
            vmem(w_query.shape, BF16), vmem(w_key.shape, BF16), vmem(w_value.shape, BF16), vmem(w_out.shape, BF16),
            vmem(ws_gate.shape, BF16), vmem(ws_up.shape, BF16), vmem(ws_down.shape, BF16),
            vmem(we_gate.shape, BF16), vmem(we_up.shape, BF16), vmem(we_down.shape, BF16),
            vmem((SLOTS, BLK, kv_width, seq_len), BF16), vmem((SLOTS, BLK, kv_width, seq_len), BF16),
            vmem((3, rows, width), BF16), vmem((3, top_k, rows), jnp.int32), vmem((3, top_k, rows), F32),
            vmem((rows, width), BF16), vmem((rows, q_w + 2 * kv_width + 128), BF16), vmem((rows, q_w), BF16),
            vmem((rows, width), F32), vmem((rows, width), F32), vmem((we_gate.shape[0], rows, 128), F32),
            vmem((rows, width), BF16), vmem((rows, width), BF16), vmem((rows, width), BF16), vmem((rows, width), BF16),
            vmem((rows, width), BF16), vmem((rows, width), BF16), vmem((rows, width), BF16), vmem((rows, width), BF16),
            vmem((rows, width), F32),
            dma((6,)), dma((q_w // head_dim,)), dma((3,)), dma((SLOTS,)), dma((SLOTS,)),
            dma((3, 3)), dma((3, 3)), dma((1,)), dma((1,)), dma((1,)), dma((1,)),
            dma((n_chunks,)), dma((n_chunks,)), dma((n_chunks,)), dma((n_chunks,)), dma((n_chunks,)),
        ]
        in_vmem = pl.BlockSpec(memory_space=pltpu.VMEM)
        anywhere = pl.BlockSpec(memory_space=pl.ANY)
        return pl.pallas_call(
            layer_kernel,
            out_shape=jax.ShapeDtypeStruct((rows, width), BF16),
            in_specs=[in_vmem] * 5 + [anywhere] * 12,
            out_specs=anywhere,
            scratch_shapes=scratch,
            compiler_params=pltpu.CompilerParams(collective_id=0, has_side_effects=True, vmem_limit_bytes=67043328),
            name="moe_layer",
        )(hidden, expert_ids.T, route_gates.T, lengths.reshape(1, rows), norm_gain.reshape(1, width), k_t, v_t, w_query, w_key, w_value, w_out, ws_gate, ws_up, ws_down, we_gate, we_up, we_down)

    return jax.shard_map(device_body, mesh=mesh, in_specs=in_specs, out_specs=tok_rows, check_vma=False)
```

```python
import functools

import jax
import jax.numpy as jnp
from jax import lax
from jax.experimental import pallas as pl
from jax.experimental.pallas import tpu as pltpu
from jax.sharding import PartitionSpec as P

NORM_EPS = 1e-6
F32 = jnp.float32
BF16 = jnp.bfloat16
MESH = pl.DeviceIdType.MESH

BLK = 16
SLOTS = 4
CHUNK = 64
LAG = 4
HEAD_BLOCKS = 8


def layer_kernel(
    h_ref, ids_ref, gates_ref, lens_ref, gain_ref, k_hbm, v_hbm, wq_hbm, wk_hbm, wv_hbm, wo_hbm, wsg_hbm, wsu_hbm, wsd_hbm,
    weg_hbm, weu_hbm, wed_hbm,
    out_hbm,
    wq, wk, wv, wo, wsg, wsu, wsd, weg, weu, wed, kbuf, vbuf,
    h_in, ids_in, gates_in, xs, aug, qdiag, heads, vflip, acc, dpart, cwb,
    psend, precv, dsend, drecv, xsend, xrecv, ysend, yrecv,
    wsem, wosem, esem, ksem, vsem, hs_send, hs_recv, p_send, p_recv, d_send, d_recv, x_send, x_recv, y_send, y_recv, osem,
):
    tp = lax.axis_index("tp")
    ep = lax.axis_index("ep")
    dp = lax.axis_index("dp")
    core = lax.rem(ep, 2)
    chip = ep // 2
    partner = (dp, tp, 2 * chip + 1 - core)
    xnbr = (dp, tp, 2 * (1 - chip) + core)
    ynbr = (dp, 1 - tp, ep)

    rows = h_ref.shape[0]
    n_blocks = rows // BLK
    n_chunks = rows // CHUNK
    kv_width = wk.shape[1]
    n_local = weg.shape[0]
    n_heads = wq.shape[1] // 64
    seq_len = kbuf.shape[3]

    small = [(wq_hbm, wq), (wk_hbm, wk), (wv_hbm, wv), (wsg_hbm, wsg), (wsu_hbm, wsu), (wsd_hbm, wsd)]
    small_copies = [pltpu.make_async_copy(s, d, wsem.at[i]) for i, (s, d) in enumerate(small)]
    for c in small_copies:
        c.start()
    barrier = pltpu.get_barrier_semaphore()
    for dev in (partner, xnbr, ynbr):
        pl.semaphore_signal(barrier, inc=1, device_id=dev, device_id_type=MESH)
    big_copies = [pltpu.make_async_copy(s, d, esem.at[i]) for i, (s, d) in enumerate(((weg_hbm, weg), (weu_hbm, weu), (wed_hbm, wed)))]
    for c in big_copies:
        c.start()
    def remote(src, dst, ssem, rsem, dev):
        return pltpu.make_async_remote_copy(src_ref=src, dst_ref=dst, send_sem=ssem, recv_sem=rsem, device_id=dev, device_id_type=MESH)

    def half_rows(m):
        return pl.ds(pl.multiple_of(m * (rows // 2), rows // 2), rows // 2)

    def row_copy(src, slot, m, dev):
        return remote(src.at[half_rows(m)], h_in.at[slot, half_rows(m)], hs_send.at[slot, m], hs_recv.at[slot, m], dev)

    def route_copies(ids, gates, slot, dev):
        pairs = ((ids, ids_in.at[slot]), (gates, gates_in.at[slot]))
        return [remote(s, d, hs_send.at[slot, 2 + i], hs_recv.at[slot, 2 + i], dev) for i, (s, d) in enumerate(pairs)]

    routes = [
        route_copies(ids_ref, gates_ref, 0, partner),
        route_copies(ids_ref, gates_ref, 1, xnbr),
        route_copies(ids_in.at[1], gates_in.at[1], 2, partner),
    ]

    def rows_to_partner(m):
        return row_copy(h_ref, 0, m, partner)

    def rows_to_xnbr(m):
        return row_copy(h_ref, 1, m, xnbr)

    def rows_forward(m):
        return row_copy(h_in.at[1], 2, m, partner)

    wo_copies = []
    for i in range(n_heads):
        dst_row = (i % 2) * kv_width + (i // 2) * 64
        wo_copies.append(pltpu.make_async_copy(wo_hbm.at[pl.ds(i * 64, 64), :], wo.at[pl.ds(dst_row, 64), :], wosem.at[i]))

    def kv_copies(b, slot):
        start = pl.multiple_of(b * BLK, BLK)
        return (
            pltpu.make_async_copy(k_hbm.at[pl.ds(start, BLK)], kbuf.at[slot], ksem.at[slot]),
            pltpu.make_async_copy(v_hbm.at[pl.ds(start, BLK)], vbuf.at[slot], vsem.at[slot]),
        )

    half = rows // 2

    def normalize(src, m):
        for i in range(half // 64):
            hf = src[pl.ds(m * half + i * 64, 64), :].astype(F32)
            inv = lax.rsqrt(jnp.mean(hf * hf, axis=1, keepdims=True) + NORM_EPS)
            xs[m, i * 64 : i * 64 + 64, :] = (hf * inv * gain_ref[...]).astype(BF16)

    def gate_weights(table, ids, gates):
        first = ep * (2 * n_local) + tp * n_local
        expert = first + lax.broadcasted_iota(jnp.int32, (8, half), 0)
        total = jnp.zeros((8, half), F32)
        for j in range(ids.shape[0]):
            total += jnp.where(ids[j : j + 1, :] == expert, gates[j : j + 1, :], 0.0)
        cols = total.T
        for e in range(n_local):
            cwb[table, e] = jnp.broadcast_to(cols[:, e : e + 1], (half, 128))

    def experts(dst, dst_row, m, table):
        d = pl.ds(dst_row, half)

        @pl.loop(0, n_local // 2)
        def _(i):
            x = xs[m]
            total = dst[d, :]
            hids = []
            for k in range(2):
                gate = jnp.dot(x, weg[2 * i + k], preferred_element_type=F32)
                up = jnp.dot(x, weu[2 * i + k], preferred_element_type=F32)
                hids.append((gate * jax.nn.sigmoid(gate) * up).astype(BF16))
            for k in range(2):
                y = jnp.dot(hids[k], wed[2 * i + k], preferred_element_type=F32)
                total = total + jnp.tile(cwb[table, 2 * i + k], (1, y.shape[1] // 128)) * y
            dst[d, :] = total

    for m in range(2):
        normalize(h_ref, m)
    for c in small_copies:
        c.wait()
    for b in range(SLOTS):
        for c in kv_copies(b, b):
            c.start()
    for c in wo_copies:
        c.start()

    col = lax.broadcasted_iota(jnp.int32, (n_heads * 64, n_heads * 64), 1)
    row = lax.broadcasted_iota(jnp.int32, (n_heads * 64, n_heads * 64), 0)
    src_row = ((lax.rem(col, kv_width) // 64) * 2 + col // kv_width) * 64 + lax.rem(col, 64)
    perm = (row == src_row).astype(F32).astype(BF16)
    lens = jnp.broadcast_to(lens_ref[...], (8, rows)).astype(F32).T
    q_w = n_heads * 64
    R8 = BLK * n_heads
    rep = (lax.broadcasted_iota(jnp.int32, (R8, BLK), 0) // n_heads == lax.broadcasted_iota(jnp.int32, (R8, BLK), 1)).astype(F32).astype(BF16)
    r_i = lax.broadcasted_iota(jnp.int32, (R8, kv_width), 0)
    c_i = lax.broadcasted_iota(jnp.int32, (R8, kv_width), 1)
    own_head = lax.rem(r_i, n_heads) // 2 == c_i // 64
    even = lax.rem(r_i, 2) == 0
    for m in range(2):
        r = pl.ds(m * half, half)
        x = xs[m]
        q = jnp.dot(x, wq[...], preferred_element_type=F32).astype(BF16)
        qp = jnp.dot(q, perm, preferred_element_type=F32).astype(BF16)
        for g in range(2):
            heads[pl.ds(g * rows + m * half, half), :] = qp[:, g * kv_width : (g + 1) * kv_width]
        aug[r, 0:kv_width] = jnp.dot(x, wk[...], preferred_element_type=F32).astype(BF16)
        aug[r, kv_width : 2 * kv_width] = jnp.dot(x, wv[...], preferred_element_type=F32).astype(BF16)
        aug[r, 2 * kv_width : 2 * kv_width + 128] = jnp.broadcast_to(lens[m * half : (m + 1) * half, 0:1], (half, 128)).astype(BF16)
        gate = jnp.dot(x, wsg[...], preferred_element_type=F32)
        up = jnp.dot(x, wsu[...], preferred_element_type=F32)
        hid = (gate * jax.nn.sigmoid(gate) * up).astype(BF16)
        acc[r, :] = jnp.dot(hid, wsd[...], preferred_element_type=F32)

    pl.semaphore_wait(barrier, 3)
    for c in routes[1] + routes[0] + [rows_to_xnbr(0), rows_to_partner(0), rows_to_xnbr(1), rows_to_partner(1)]:
        c.start()

    @pl.loop(0, n_blocks // 8)
    def _(i):
        for k in range(8):
            b = 8 * i + k
            both = [jnp.dot(rep, heads[pl.ds(pl.multiple_of(g * rows + b * BLK, BLK), BLK), :], preferred_element_type=F32) for g in range(2)]
            mine = jnp.where(even, both[0], both[1])
            qdiag[pl.ds(pl.multiple_of(b * R8, R8), R8), :] = jnp.where(own_head, mine, 0.0).astype(BF16)

    n_pairs = BLK // 2

    def attend_pair(b0):
        slots = [lax.rem(b0 + j, SLOTS) for j in range(2)]
        for j in range(2):
            for c in kv_copies(b0 + j, slots[j]):
                c.wait()
        scores, news, sums = [], [], []
        for j in range(2):
            parts = []
            for t in range(BLK):
                vflip[j, t] = vbuf[slots[j], t].T
            for p in range(n_pairs):
                lhs = qdiag[pl.ds(pl.multiple_of((b0 + j) * R8 + 16 * p, 16), 16), :]
                parts.append(jnp.dot(lhs, kbuf[slots[j], 2 * p], preferred_element_type=F32)[0:8])
                parts.append(jnp.dot(lhs, kbuf[slots[j], 2 * p + 1], preferred_element_type=F32)[8:16])
            scores.append(jnp.concatenate(parts, axis=0) * 0.125)
        for j in range(2):
            news.append(jnp.dot(rep, aug[pl.ds(pl.multiple_of((b0 + j) * BLK, BLK), BLK), :], preferred_element_type=F32))
        weights = []
        for j in range(2):
            full = news[j]
            qf = qdiag[pl.ds(pl.multiple_of((b0 + j) * R8, R8), R8), :].astype(F32)
            s_new = jnp.sum(qf * full[:, 0:kv_width], axis=1, keepdims=True) * 0.125
            ln = full[:, 2 * kv_width : 2 * kv_width + 128]
            pos = lax.broadcasted_iota(jnp.int32, (R8, seq_len), 1).astype(F32)
            s = jnp.where(pos < jnp.tile(ln, (1, seq_len // 128)), scores[j], -1e30)
            top = jnp.maximum(jnp.max(s, axis=1, keepdims=True), s_new)
            w = jnp.exp(s - top)
            w_new = jnp.exp(s_new - top)
            sums.append((w_new, jnp.sum(w, axis=1, keepdims=True) + w_new))
            weights.append(w.astype(BF16))
        for j in range(2):
            parts = []
            for p in range(n_pairs):
                lhs = weights[j][16 * p : 16 * p + 16]
                parts.append(jnp.dot(lhs, vflip[j, 2 * p], preferred_element_type=F32)[0:8])
                parts.append(jnp.dot(lhs, vflip[j, 2 * p + 1], preferred_element_type=F32)[8:16])
            w_new, den = sums[j]
            num = jnp.concatenate(parts, axis=0) + w_new * news[j][:, kv_width : 2 * kv_width]
            heads[pl.ds(pl.multiple_of((b0 + j) * R8, R8), R8), :] = jnp.where(own_head, num / den, 0.0).astype(BF16)

    def attend_blocks(first, count):
        @pl.loop(0, count // 2)
        def _(i):
            b = first + 2 * i
            attend_pair(b)

            @pl.when(b + SLOTS < n_blocks)
            def _():
                for j in range(2):
                    for c in kv_copies(b + j + SLOTS, lax.rem(b + j, SLOTS)):
                        c.start()

    def half_copy(src, dst, ssem, rsem, m):
        r = pl.ds(m * half, half)
        return remote(src.at[r, :], dst.at[r, :], ssem.at[m], rsem.at[m], partner)

    def wait_recv(copies):
        for c in copies:
            c.wait_recv()

    for c in big_copies:
        c.wait()

    @pl.loop(0, 2)
    def _(m):
        gate_weights(0, ids_ref[:, half_rows(m)], gates_ref[:, half_rows(m)])
        experts(acc, m * half, m, 0)
        attend_blocks(4 * m, 4)

    for c in routes[1]:
        c.wait_recv()
    for c in routes[2]:
        c.start()
    for c in routes[0] + routes[2]:
        c.wait_recv()

    def chunk_copy(src, dst, ssem, rsem, c, dev):
        r = pl.ds(pl.multiple_of(c * CHUNK, CHUNK), CHUNK)
        return remote(src.at[r, :], dst.at[r, :], ssem.at[c], rsem.at[c], dev)

    for c in wo_copies:
        c.wait()

    def out_copy(c):
        r = pl.ds(pl.multiple_of(c * CHUNK, CHUNK), CHUNK)
        q = pl.ds(pl.multiple_of(lax.rem(c, n_chunks // 2) * CHUNK, CHUNK), CHUNK)
        return pltpu.make_async_copy(xs.at[c // (n_chunks // 2), q, :], out_hbm.at[r, :], osem.at[c])

    def finish(c):
        r = pl.ds(pl.multiple_of(c * CHUNK, CHUNK), CHUNK)
        chunk_copy(ysend, yrecv, y_send, y_recv, c, ynbr).wait_recv()
        both = ysend[r, :].astype(F32) + yrecv[r, :].astype(F32)
        q = pl.ds(pl.multiple_of(lax.rem(c, n_chunks // 2) * CHUNK, CHUNK), CHUNK)
        xs[c // (n_chunks // 2), q, :] = (h_ref[r, :].astype(F32) + both).astype(BF16)
        out_copy(c).start()

    rows_c = CHUNK * n_heads
    g_r = lax.broadcasted_iota(jnp.int32, (2 * CHUNK, rows_c), 0)
    g_c = lax.broadcasted_iota(jnp.int32, (2 * CHUNK, rows_c), 1)
    fold = ((g_c // n_heads == lax.rem(g_r, CHUNK)) & (lax.rem(g_c, 2) == g_r // CHUNK)).astype(F32).astype(BF16)

    def combine(c):
        r = pl.ds(pl.multiple_of(c * CHUNK, CHUNK), CHUNK)
        o = jnp.dot(fold, heads[pl.ds(pl.multiple_of(c * rows_c, rows_c), rows_c), :], preferred_element_type=F32).astype(BF16)
        attn = jnp.dot(o[0:CHUNK], wo[0:kv_width, :], preferred_element_type=F32) + jnp.dot(o[CHUNK : 2 * CHUNK], wo[kv_width : 2 * kv_width, :], preferred_element_type=F32)
        chunk_copy(xsend, xrecv, x_send, x_recv, c, xnbr).wait_recv()
        ysend[r, :] = (acc[r, :] + attn + precv[r, :].astype(F32) + xrecv[r, :].astype(F32)).astype(BF16)
        chunk_copy(ysend, yrecv, y_send, y_recv, c, ynbr).start()

    def remote_unit(slot, m, table):
        gate_weights(table, ids_in[slot, :, half_rows(m)], gates_in[slot, :, half_rows(m)])
        normalize(h_in.at[slot], m)
        dpart[...] = jnp.zeros_like(dpart)
        experts(dpart, 0, m, table)

    first_chunks = n_chunks // 2

    @pl.loop(0, 2)
    def _(m):
        r = half_rows(m)
        b = HEAD_BLOCKS + 8 * m

        def early(c):
            @pl.when(m == 1)
            def _():
                if c == 0:
                    half_copy(psend, precv, p_send, p_recv, 0).wait_recv()
                combine(c)

        rows_to_xnbr(m).wait_recv()
        rows_forward(m).start()
        attend_blocks(b, 2)
        early(0)
        rows_forward(m).wait_recv()
        remote_unit(2, m, 0)
        dsend[r, :] = dpart[...].astype(BF16)
        half_copy(dsend, drecv, d_send, d_recv, m).start()
        early(1)
        attend_blocks(b + 2, 2)
        early(2)
        remote_unit(1, m, 1)
        half_copy(dsend, drecv, d_send, d_recv, m).wait_recv()
        xsend[r, :] = (dpart[...] + drecv[r, :].astype(F32)).astype(BF16)
        for i in range(first_chunks):
            chunk_copy(xsend, xrecv, x_send, x_recv, m * first_chunks + i, xnbr).start()
        attend_blocks(b + 4, 2)
        early(3)
        rows_to_partner(m).wait_recv()
        remote_unit(0, m, 2)
        psend[r, :] = dpart[...].astype(BF16)
        half_copy(psend, precv, p_send, p_recv, m).start()
        attend_blocks(b + 6, 2)

    half_copy(psend, precv, p_send, p_recv, 1).wait_recv()

    @pl.loop(first_chunks, n_chunks)
    def _(c):
        attend_blocks(HEAD_BLOCKS + 16 + 2 * (c - first_chunks), 2)
        combine(c)
        finish(c - LAG)

    for c in range(n_chunks - LAG, n_chunks):
        finish(c)

    for c in routes[0] + routes[1] + routes[2]:
        c.wait_send()
    for m in range(2):
        for c in (rows_to_partner(m), rows_to_xnbr(m), rows_forward(m)):
            c.wait_send()
        half_copy(psend, precv, p_send, p_recv, m).wait_send()
        half_copy(dsend, drecv, d_send, d_recv, m).wait_send()

    @pl.loop(0, n_chunks)
    def _(c):
        r = pl.ds(pl.multiple_of(c * CHUNK, CHUNK), CHUNK)
        chunk_copy(xsend, xrecv, x_send, x_recv, c, xnbr).wait_send()
        chunk_copy(ysend, yrecv, y_send, y_recv, c, ynbr).wait_send()
        out_copy(c).wait()


def solution(mesh):
    tok_rows = P(("dp", "ep"), None)
    cache_spec = P(("dp", "ep"), None, "tp", None)
    col_split = P(None, "tp")
    row_split = P("tp", None)
    exp_split = P(("ep", "tp"), None, None)
    in_specs = (tok_rows, cache_spec, cache_spec, P(("dp", "ep")), tok_rows, tok_rows, P(None), col_split, col_split, col_split, row_split, col_split, col_split, row_split, exp_split, exp_split, exp_split)

    def device_body(hidden, k_cache, v_cache, lengths, expert_ids, route_gates, norm_gain, w_query, w_key, w_value, w_out, ws_gate, ws_up, ws_down, we_gate, we_up, we_down):
        rows, width = hidden.shape
        seq_len, kv_local, head_dim = k_cache.shape[1:]
        kv_width = kv_local * head_dim
        top_k = expert_ids.shape[1]
        k_t = k_cache.transpose(0, 2, 3, 1).reshape(rows, kv_width, seq_len)
        v_t = v_cache.transpose(0, 2, 3, 1).reshape(rows, kv_width, seq_len)
        n_chunks = rows // CHUNK
        q_w = w_query.shape[1]
        dma = pltpu.SemaphoreType.DMA
        vmem = pltpu.VMEM
        scratch = [
            vmem(w_query.shape, BF16), vmem(w_key.shape, BF16), vmem(w_value.shape, BF16), vmem(w_out.shape, BF16),
            vmem(ws_gate.shape, BF16), vmem(ws_up.shape, BF16), vmem(ws_down.shape, BF16),
            vmem(we_gate.shape, BF16), vmem(we_up.shape, BF16), vmem(we_down.shape, BF16),
            vmem((SLOTS, BLK, kv_width, seq_len), BF16), vmem((SLOTS, BLK, kv_width, seq_len), BF16),
            vmem((3, rows, width), BF16), vmem((3, top_k, rows), jnp.int32), vmem((3, top_k, rows), F32),
            vmem((2, rows // 2, width), BF16), vmem((rows, 2 * kv_width + 128), BF16),
            vmem((rows * q_w // head_dim, kv_width), BF16), vmem((rows * q_w // head_dim, kv_width), BF16),
            vmem((2, BLK, seq_len, kv_width), BF16),
            vmem((rows, width), F32), vmem((rows // 2, width), F32), vmem((3, we_gate.shape[0], rows // 2, 128), F32),
            vmem((rows, width), BF16), vmem((rows, width), BF16), vmem((rows, width), BF16), vmem((rows, width), BF16),
            vmem((rows, width), BF16), vmem((rows, width), BF16), vmem((rows, width), BF16), vmem((rows, width), BF16),
            dma((6,)), dma((q_w // head_dim,)), dma((3,)), dma((SLOTS,)), dma((SLOTS,)),
            dma((3, 4)), dma((3, 4)), dma((2,)), dma((2,)), dma((2,)), dma((2,)),
            dma((n_chunks,)), dma((n_chunks,)), dma((n_chunks,)), dma((n_chunks,)), dma((n_chunks,)),
        ]
        in_vmem = pl.BlockSpec(memory_space=pltpu.VMEM)
        anywhere = pl.BlockSpec(memory_space=pl.ANY)
        return pl.pallas_call(
            layer_kernel,
            out_shape=jax.ShapeDtypeStruct((rows, width), BF16),
            in_specs=[in_vmem] * 5 + [anywhere] * 12,
            out_specs=anywhere,
            scratch_shapes=scratch,
            compiler_params=pltpu.CompilerParams(collective_id=0, has_side_effects=True, vmem_limit_bytes=67043328),
            name="moe_layer",
        )(hidden, expert_ids.T, route_gates.T, lengths.reshape(1, rows), norm_gain.reshape(1, width), k_t, v_t, w_query, w_key, w_value, w_out, ws_gate, ws_up, ws_down, we_gate, we_up, we_down)

    return jax.shard_map(device_body, mesh=mesh, in_specs=in_specs, out_specs=tok_rows, check_vma=False)
```
